256 devices in a mesh: groups: 2 (over z), expert: 16 (over x, core), cuts: 8 (over y).
Axes of the slice: x: 8, y: 8, z: 2, core: 2. Of those that a mesh axis runs over, the one named last changes fastest.
The devices are a block of a 8x8x16 slice.
Arguments:
- tokens: bfloat16 [16384, 2048], P(('groups', 'expert')), parts along dimension 0, may hold values from -6 to 6
- route: int32 [16384, 1], P(('groups', 'expert')), parts along dimension 0, may hold values from 0 to 15; in each aligned block of 512 rows (0 to 511, 512 to 1023, ...) at most 48 rows name the same one
- gate_prob: float32 [16384], P(('groups', 'expert')), parts along dimension 0, may hold values from 0.2 to 1
- norm_gain: float32 [2048], replicated, may hold values from 0.5 to 1.5
- dense_in: bfloat16 [2048, 8192], P('expert', 'cuts'), may hold values from -0.125 to 0.125
- dense_out: bfloat16 [8192, 2048], P('cuts', 'expert'), may hold values from -0.0625 to 0.0625
- expert_in: bfloat16 [16, 2048, 8192], P('expert', None, 'cuts'), may hold values from -0.125 to 0.125
- expert_out: bfloat16 [16, 8192, 2048], P('expert', 'cuts'), may hold values from -0.0625 to 0.0625
Outputs:
- layer_out: bfloat16 [16384, 2048], P(('groups', 'expert'), 'cuts'), parts along dimension 0
The draws below stay inside these ranges and needn't reach their ends.
There are 2 independent parts, one for each index of `groups`. The reference program is written for one: setup_inputs(seed, part) draws one part's arguments, and reference() takes and returns one part's arrays. A program takes and returns all parts, laid end to end along the dimension named above; an argument that names none is the same for every part. Nothing has to cross between parts.
Inputs may be any that keep to these rules, and one draw needn't show every extreme that they name: `route`: within the rows of one device (aligned blocks of 512 rows) no expert is named by more than 48 rows; in some blocks one expert is named by exactly 48 rows.
All inputs are finite; a program needn't handle non-finite values.
Results may differ from the reference program's by a relative error of at most 0.0095.
Values may be sent and summed in bfloat16 or wider, within the bound.
No kernel may reach another device: no remote copies, remote signals or barrier semaphores. Data moves between devices by JAX's collectives and lax.ppermute only.
A program may use at most 64 MiB of HBM per device.

```python
import math
import jax
import jax.numpy as jnp
import numpy as np
from jax import lax

D = 2048
FF = 8192
TOK_E = 512
EXPERTS = 16
CAP = 48
TOKENS = 8192
N_EXPERT = 16
N_CUTS = 8


def levels(stream_key, dims, shards, least, top_value):
    def one(dim, shards_of):
        draws = jax.random.uniform(jax.random.fold_in(jax.random.fold_in(stream_key, 6), dim), (shards_of,), jnp.float32, least / len(shards), top_value / len(shards))
        return jnp.repeat(jnp.exp(draws), dims[dim] // shards_of).reshape((-1,) + (1,) * (len(dims) - dim - 1))

    factor_of = one(*shards[0])
    for cut in shards[1:]:
        factor_of = factor_of * one(*cut)
    return factor_of


def shared_out(stream_key, own, number, rows, amount, top, limit, skew):
    sequence = jax.random.permutation(stream_key, amount)
    crowded, usual = portions_of(amount, rows * top, limit, skew, True), portions_of(amount, rows * top, limit, skew, False)
    places = jnp.arange(amount)

    def named(tallies, rotation):
        used = int((tallies > 0).sum())
        fixed = max(1, used // 4)
        shifted = fixed + (places - fixed + rotation * (used - fixed)) % max(1, amount - fixed)
        return jnp.zeros((amount,), jnp.int32).at[sequence[jnp.where(places < fixed, places, shifted)]].set(jnp.asarray(tallies, jnp.int32))

    tallies = jnp.where(number % 4 == 0, named(crowded, number // 4), named(usual, number - number // 4 - 1))
    mixed = jax.random.permutation(jax.random.fold_in(own, 3), amount)
    donor, sink = mixed[0:amount // 2 * 2:2], mixed[1:amount // 2 * 2:2]
    margin = jnp.minimum(tallies[donor] - 1, limit - tallies[sink]) // 2
    margin = jnp.where((donor == sequence[0]) | (sink == sequence[0]) | (tallies[sink] == 0), 0, jnp.maximum(margin, 0))
    shifted = jax.random.randint(jax.random.fold_in(own, 4), (amount // 2,), 0, 1 << 20) % (margin + 1)
    tallies = tallies.at[donor].add(-shifted).at[sink].add(shifted)
    items = jnp.searchsorted(jnp.cumsum(tallies), jnp.arange(rows * top), side="right").astype(jnp.int32)
    listing = items.reshape(top, rows).T
    listing = listing[jax.random.permutation(jax.random.fold_in(own, 1), rows)]
    rotation = jax.random.randint(jax.random.fold_in(own, 2), (rows, 1), 0, top)
    return jnp.take_along_axis(listing, (jnp.arange(top)[None, :] + rotation) % top, axis=1)


def portions_of(number_of, total, reach, skew, full):
    weights = [(1 << 20) // math.isqrt(rank ** skew) + 1 for rank in range(1, number_of + 1)]
    largest = reach if full else min(reach, max(-(-total // number_of), total * weights[0] // sum(weights)))
    least = 1 if total - largest >= number_of - 1 else 0
    counts, surplus = [largest] + [least] * (number_of - 1), total - largest - least * (number_of - 1)
    while surplus > 0:
        free = [i for i in range(1, number_of) if counts[i] < largest] or [i for i in range(1, number_of) if counts[i] < reach]
        mass, left = sum([weights[i] for i in free]), surplus
        for i in free:
            more = min(reach - counts[i], max(1, left * weights[i] // mass), surplus)
            counts[i] = counts[i] + more
            surplus = surplus - more
    return np.array(counts)


def normal_values(rng, dims, deviation, bound, shards=(), kind=jnp.bfloat16):
    drawn = deviation * jax.random.normal(rng, dims, jnp.float32)
    if shards:
        drawn = drawn * levels(rng, dims, shards, -0.22, 0.18)
    return jnp.clip(drawn, -bound, bound).astype(kind)


def setup_inputs(seed: int = 0, part: int = 0) -> dict:
    arg_keys = jax.random.split(jax.random.key(seed), 9)
    part_keys = jax.random.split(jax.random.fold_in(arg_keys[8], part), 9)
    tokens = normal_values(part_keys[0], (TOKENS, D), 1.0, 6.0, ((0, 16),))
    route_keys = jax.random.split(jax.random.fold_in(part_keys[1], 1), TOKENS // TOK_E)
    route_turns = jax.random.permutation(jax.random.fold_in(part_keys[1], 3), TOKENS // TOK_E)
    route = jax.vmap(lambda own, number: shared_out(jax.random.fold_in(part_keys[1], 2), own, number, TOK_E, EXPERTS, 1, CAP, 2))(route_keys, route_turns).reshape((TOKENS, 1))
    gate_prob = jnp.clip(jnp.exp(math.log(1.0) - 1.609438 * jax.random.uniform(part_keys[2], (TOKENS,), jnp.float32) ** levels(part_keys[2], (TOKENS,), ((0, 16),), -0.2, 0.2)), 0.2, 1.0)
    norm_gain = jnp.clip(1.0 + 0.1 * jax.random.normal(arg_keys[3], (D,), jnp.float32), 0.5, 1.5)
    dense_in = normal_values(arg_keys[4], (D, FF), D ** -0.5, 0.125, ((0, 16), (1, 8)))
    dense_out = normal_values(arg_keys[5], (FF, D), FF ** -0.5, 0.0625, ((0, 8), (1, 16)))
    expert_in = normal_values(arg_keys[6], (EXPERTS, D, FF), D ** -0.5, 0.125, ((0, 16), (2, 8)))
    expert_out = normal_values(arg_keys[7], (EXPERTS, FF, D), FF ** -0.5, 0.0625, ((0, 16), (1, 8)))
    return {"tokens": tokens, "route": route, "gate_prob": gate_prob, "norm_gain": norm_gain, "dense_in": dense_in, "dense_out": dense_out, "expert_in": expert_in, "expert_out": expert_out}


def normalize(tokens, norm_gain):
    widened = tokens.astype(jnp.float32)
    meansq = lax.optimization_barrier(jnp.mean(widened * widened, axis=-1, keepdims=True))
    return (widened * lax.rsqrt(meansq + 1e-06) * norm_gain).astype(jnp.bfloat16)

def sliced_product(act, weight):
    rows = act.shape[0]
    width = FF // N_CUTS
    act_parts = act.reshape(rows, N_CUTS, width).transpose(1, 0, 2)
    weight_parts = weight.reshape(N_CUTS, width, D)

    def add_slice(total, operands):
        act_part, weight_part = operands
        partial_out = jnp.dot(act_part, weight_part, preferred_element_type=jnp.float32)
        rounded = lax.optimization_barrier(partial_out.astype(jnp.bfloat16)).astype(jnp.float32)
        return (total + rounded, None)
    total, unused = lax.scan(add_slice, jnp.zeros((rows, D), jnp.float32), (act_parts, weight_parts))
    return total

def run_expert(operands):
    gathered, weight_in, weight_out = operands
    inner = jax.nn.gelu(jnp.dot(gathered, weight_in, preferred_element_type=jnp.float32)).astype(jnp.bfloat16)
    return sliced_product(inner, weight_out).astype(jnp.bfloat16)

def reference(tokens, route, gate_prob, norm_gain, dense_in, dense_out, expert_in, expert_out):
    normed = normalize(tokens, norm_gain)
    dense_act = jax.nn.gelu(jnp.dot(normed, dense_in, preferred_element_type=jnp.float32)).astype(jnp.bfloat16)
    dense = sliced_product(dense_act, dense_out)
    picked = route[:, 0].reshape(N_EXPERT, TOK_E)
    labels = jnp.arange(EXPERTS, dtype=jnp.int32)
    one_hot = (picked[:, :, None] == labels[None, None, :]).astype(jnp.int32)
    before = jnp.cumsum(one_hot, axis=1) - one_hot
    position = lax.optimization_barrier(jnp.sum(before * one_hot, axis=-1))
    block_ids = jnp.arange(N_EXPERT, dtype=jnp.int32)[:, None]
    target = (picked * (N_EXPERT * CAP) + block_ids * CAP + position).reshape(-1).astype(jnp.int32)
    buffer = jnp.zeros((EXPERTS * N_EXPERT * CAP, D), jnp.bfloat16).at[target].set(normed)
    buffer = buffer.reshape(EXPERTS, N_EXPERT * CAP, D)
    results = lax.map(run_expert, (buffer, expert_in, expert_out)).reshape(-1, D)
    expert_res = results[target].astype(jnp.float32)
    layer_out = tokens.astype(jnp.float32) + dense + gate_prob[:, None] * expert_res
    return layer_out.astype(jnp.bfloat16)
```

```python
import jax
import jax.numpy as jnp
from jax import lax
from jax.sharding import PartitionSpec as P


def matmul(lhs, rhs):
    return jnp.dot(lhs, rhs, preferred_element_type=jnp.float32)


def wrapped(index, size):
    return jnp.where(index < 0, index + size, jnp.where(index < size, index, index - size))


def turn(values, axis, step):
    size = lax.axis_size(axis)
    return lax.ppermute(values, axis, [(i, (i + step) % size) for i in range(size)])


def ring_gather_product(own, weight, axis):
    size = lax.axis_size(axis)
    rank = lax.axis_index(axis)
    rows = own.shape[1]

    def rows_of(offset):
        return lax.dynamic_slice_in_dim(weight, wrapped(rank + offset, size) * rows, rows, 0)

    ahead = back = own
    total = matmul(own, rows_of(0))
    for hop in range(1, size // 2 + 1):
        ahead = turn(ahead, axis, 1)
        if hop <= (size - 1) // 2:
            back = turn(back, axis, -1)
            total = total + matmul(ahead, rows_of(-hop)) + matmul(back, rows_of(hop))
        else:
            total = total + matmul(ahead, rows_of(-hop))
    return total


def ring_scatter(partial_for, axis):
    size = lax.axis_size(axis)

    def chain(hops, step):
        carried = partial_for(step * hops).astype(jnp.bfloat16)
        for left in range(hops - 1, -1, -1):
            carried = turn(carried, axis, step)
            if left:
                carried = (carried.astype(jnp.float32) + partial_for(step * left)).astype(jnp.bfloat16)
        return carried.astype(jnp.float32)

    return partial_for(0) + chain(size // 2, 1) + chain((size - 1) // 2, -1)


def local(tokens, route, gate_prob, norm_gain, dense_in, dense_out, expert_in, expert_out):
    experts = lax.axis_size("expert")
    slices = lax.axis_size("cuts")
    cut = lax.axis_index("cuts")
    tok_rows, width = tokens.shape
    share = width // slices
    capacity = max(2, 3 * tok_rows // (2 * experts))
    slots = experts * capacity

    def columns(array, offset):
        return lax.dynamic_slice_in_dim(array, wrapped(cut + offset, slices) * share, share, array.ndim - 1)

    hidden = dense_in.shape[1]
    both = lax.all_gather(jnp.concatenate([dense_in, dense_out.T], axis=1), "expert", axis=0, tiled=True)
    full_in, full_out = both[:, :hidden], both[:, hidden:].T

    widened = tokens.astype(jnp.float32)
    scale = lax.rsqrt(jnp.mean(widened * widened, axis=-1, keepdims=True) + 1e-06)
    own_tokens = columns(tokens, 0).astype(jnp.float32)
    own_normed = (own_tokens * scale * columns(norm_gain, 0)).astype(jnp.bfloat16)

    picked = route[:, 0]
    one_hot = picked[:, None] == jnp.arange(experts, dtype=jnp.int32)[None, :]
    order = jnp.arange(tok_rows, dtype=jnp.int32)
    earlier = (order[None, :] < order[:, None]).astype(jnp.bfloat16)
    before = matmul(earlier, one_hot.astype(jnp.bfloat16))
    position = jnp.sum(jnp.where(one_hot, before, 0.0), axis=-1).astype(jnp.int32)
    target = picked * capacity + position
    slot_ids = jnp.arange(slots, dtype=jnp.int32)
    to_slots = (slot_ids[:, None] == target[None, :]).astype(jnp.bfloat16)
    from_slots = (target[:, None] == slot_ids[None, :]).astype(jnp.bfloat16)

    outgoing = matmul(to_slots, own_normed).astype(jnp.bfloat16)
    arrived = lax.all_to_all(
        outgoing.reshape(experts, capacity, share), "expert", split_axis=0, concat_axis=0, tiled=True
    ).reshape(slots, share)
    inner = jax.nn.gelu(ring_gather_product(arrived, expert_in[0], "cuts")).astype(jnp.bfloat16)
    weight_out = expert_out[0]
    own_share = ring_scatter(lambda offset: matmul(inner, columns(weight_out, offset)), "cuts").astype(jnp.bfloat16)
    returned = lax.all_to_all(
        own_share.reshape(experts, capacity, share), "expert", split_axis=0, concat_axis=0, tiled=True
    ).reshape(slots, share)
    expert_res = matmul(from_slots, returned)

    normed = (widened * scale * norm_gain).astype(jnp.bfloat16)
    dense_act = jax.nn.gelu(matmul(normed, full_in)).astype(jnp.bfloat16)
    dense = ring_scatter(lambda offset: matmul(dense_act, columns(full_out, offset)), "cuts")

    return (own_tokens + dense + gate_prob[:, None] * expert_res).astype(jnp.bfloat16)


def solution(mesh):
    return jax.shard_map(
        local,
        mesh=mesh,
        in_specs=(
            P(("groups", "expert"), None),
            P(("groups", "expert"), None),
            P(("groups", "expert")),
            P(),
            P("expert", "cuts"),
            P("cuts", "expert"),
            P("expert", None, "cuts"),
            P("expert", "cuts", None),
        ),
        out_specs=P(("groups", "expert"), "cuts"),
        check_vma=False,
    )
```
